32 devices in a mesh: rep: 2 (over y), ep: 16 (over z, x, core).
Axes of the slice: x: 2, y: 2, z: 4, core: 2. Of those that a mesh axis runs over, the one named last changes fastest.
Arguments:
- cache_kv: bfloat16 [64, 2048, 576], P(('rep', 'ep')), parts along dimension 0, may hold values from -6 to 6
- new_kv: bfloat16 [64, 2, 576], P(('rep', 'ep')), parts along dimension 0, may hold values from -6 to 6
- queries: bfloat16 [64, 2, 64, 576], P(('rep', 'ep')), parts along dimension 0, may hold values from -256 to 256
- lengths: int32 [64], P(('rep', 'ep')), parts along dimension 0, may hold values from 256 to 2048
- resid: bfloat16 [64, 2, 7168], P(('rep', 'ep')), parts along dimension 0, may hold values from -18 to 18
- value_up: bfloat16 [512, 8192], P(None, 'ep'), may hold values from -1.5 to 1.5
- out_proj: bfloat16 [8192, 7168], P('ep'), may hold values from -0.09375 to 0.09375
- norm_gain: bfloat16 [7168], replicated, may hold values from 0.25 to 1.75
- router: bfloat16 [7168, 16], replicated, may hold values from -0.0625 to 0.0625
- expert_ids: int32 [64, 2, 8], P(('rep', 'ep')), parts along dimension 0, may hold values from 0 to 15, as said below
- slots: int32 [64, 2, 8], P(('rep', 'ep')), parts along dimension 0, may hold values from 0 to 3, as said below
- w_gate: bfloat16 [7168, 16384], P(None, 'ep'), may hold values from -0.0625 to 0.0625
- w_up: bfloat16 [7168, 16384], P(None, 'ep'), may hold values from -0.0625 to 0.0625
- w_down: bfloat16 [16384, 7168], P('ep'), may hold values from -0.1875 to 0.1875
Outputs:
- mixed: bfloat16 [64, 2, 7168], P(('rep', 'ep')), parts along dimension 0
The draws below stay inside these ranges and needn't reach their ends.
There are 2 independent parts, one for each index of `rep`. The reference program is written for one: setup_inputs(seed, part) draws one part's arguments, and reference() takes and returns one part's arrays. A program takes and returns all parts, laid end to end along the dimension named above; an argument that names none is the same for every part. Nothing has to cross between parts.
Inputs may be any that keep to these rules, and one draw needn't show every extreme that they name: `expert_ids`: each row names 8 different experts. In each aligned block of 4 rows (the rows of one device), the rows that name the same expert carry the distinct slots 0 up to their number minus one for it; in every block some expert is named by all 4 rows.
All inputs are finite; a program needn't handle non-finite values.
Results may differ from the reference program's by a relative error of at most 0.0065.
Values may be sent and summed in bfloat16 or wider, within the bound.
A program may use at most 128 MiB of HBM per device.

```python
import jax
import jax.numpy as jnp
from jax import lax

D = 7168
H = 64
LAT = 512
VH = 128
FFW = 1024
EXPERTS = 16
TOP = 8
CAP = 2
STEPS = 2
CACHE = 2048
KV = 576
QK = 192
TOK_DEV = 4
BATCH = 32
N_EP = 16


def attention_pair(key):
    cache_part = jax.random.truncated_normal(jax.random.fold_in(key, 21), -6.0, 6.0, (BATCH, CACHE, KV), jnp.float32)
    query_part = jax.random.truncated_normal(jax.random.fold_in(key, 22), -6.0, 6.0, (BATCH, STEPS, H, KV), jnp.float32)
    return (cache_part, query_part)


def draw_cache_kv(key, part):
    return attention_pair(key)[0].astype(jnp.bfloat16)


def draw_queries(key, part):
    return attention_pair(key)[1].astype(jnp.bfloat16)


def draw_resid(key, part):
    columns = jnp.exp(jax.random.uniform(jax.random.fold_in(key, 31), (D,), jnp.float32, jnp.log(0.3), jnp.log(3.0)))
    base = jax.random.truncated_normal(jax.random.fold_in(key, 34), -6.0, 6.0, (BATCH, STEPS, D), jnp.float32)
    return (base * columns).astype(jnp.bfloat16)


def routing_pair(key):
    rows_all = BATCH * STEPS
    blocks = rows_all // TOK_DEV
    expert_range = jnp.arange(EXPERTS, dtype=jnp.int32)
    base = jax.random.randint(jax.random.fold_in(key, 41), (rows_all, EXPERTS), 0, 1 << 20)
    order = jax.random.permutation(jax.random.fold_in(key, 42), EXPERTS).astype(jnp.int32)
    forced = jax.random.randint(jax.random.fold_in(key, 43), (blocks,), 0, EXPERTS)
    forced_rows = jnp.repeat(forced, TOK_DEV)
    boost = jnp.where(expert_range[None, :] == forced_rows[:, None], 1 << 24, 0)
    scores = (base + order[None, :] * (1 << 16) + boost) * EXPERTS + expert_range[None, :]
    _, chosen = lax.top_k(scores, TOP)
    chosen = chosen.astype(jnp.int32)
    row_in_block = jnp.arange(rows_all, dtype=jnp.int32) % TOK_DEV
    priority = jax.random.randint(jax.random.fold_in(key, 44), (rows_all, EXPERTS), 0, 1 << 20) * TOK_DEV + row_in_block[:, None]
    named = jnp.any(chosen[:, :, None] == expert_range[None, None, :], axis=1)
    named_block = named.reshape(blocks, TOK_DEV, EXPERTS)
    priority_block = priority.reshape(blocks, TOK_DEV, EXPERTS)
    earlier = named_block[:, None, :, :] & (priority_block[:, None, :, :] < priority_block[:, :, None, :])
    rank = jnp.sum(earlier.astype(jnp.int32), axis=2).reshape(rows_all, EXPERTS)
    slot_values = jnp.take_along_axis(rank, chosen, axis=1)
    return (chosen.reshape(BATCH, STEPS, TOP), slot_values.reshape(BATCH, STEPS, TOP))


def draw_expert_ids(key, part):
    return routing_pair(key)[0]


def draw_slots(key, part):
    return routing_pair(key)[1]


def set_ends(drawn, rng, least, high):
    longest = drawn.shape.index(max(drawn.shape))
    spots = []
    for shift in (0, 1):
        where = [jax.random.randint(jax.random.fold_in(rng, axis), (), 0, length) for axis, length in enumerate(drawn.shape)]
        where[longest] = (where[longest] + shift) % drawn.shape[longest]
        spots.append(tuple(where))
    return drawn.at[spots[0]].set(least).at[spots[1]].set(high)


def steps_of(rng, extent, cuts, smallest, top_value):
    factor_of, own = 1.0, jax.random.fold_in(rng, 6)
    for position, blocks in cuts:
        steps = jnp.exp(jax.random.uniform(jax.random.fold_in(own, position), (blocks,), jnp.float32, smallest / len(cuts), top_value / len(cuts)))
        factor_of = factor_of * jnp.repeat(steps, extent[position] // blocks).reshape([-1 if axis == position else 1 for axis in range(len(extent))])
    return factor_of


def normal_values(own_key, dims, deviation, bound, pieces=(), held_as=jnp.bfloat16):
    loudness = steps_of(own_key, dims, pieces, -0.22, 0.18) if pieces else 1.0
    values = jax.random.normal(own_key, dims, jnp.float32) * deviation * loudness
    return jnp.minimum(jnp.maximum(values, -bound), bound).astype(held_as)


def setup_inputs(seed: int = 0, part: int = 0) -> dict:
    key_list = jax.random.split(jax.random.key(seed), 15)
    part_splits = jax.random.split(jax.random.fold_in(key_list[14], part), 15)
    cache_kv = draw_cache_kv(jax.random.fold_in(jax.random.fold_in(key_list[14], part), 71), part)
    new_kv = normal_values(part_splits[1], (BATCH, STEPS, KV), 1.0, 6.0, ((0, 16),))
    queries = draw_queries(jax.random.fold_in(jax.random.fold_in(key_list[14], part), 71), part)
    lengths = set_ends(jax.random.randint(part_splits[3], (BATCH,), CACHE // 8, CACHE + 1), jax.random.fold_in(part_splits[3], 1), CACHE // 8, CACHE).astype(jnp.int32)
    resid = draw_resid(jax.random.fold_in(jax.random.fold_in(key_list[14], part), 71), part)
    value_up = normal_values(key_list[5], (LAT, H * VH), (max(1, LAT // 32)) ** -0.5, 1.5, ((1, 16),))
    out_proj = normal_values(key_list[6], (H * VH, D), (H * VH // 2) ** -0.5, 0.09375, ((0, 16),))
    norm_gain = jnp.clip(1.0 + 0.15 * jax.random.normal(key_list[7], (D,), jnp.float32), 0.25, 1.75).astype(jnp.bfloat16)
    router = normal_values(key_list[8], (D, EXPERTS), D ** -0.5, 0.0625)
    expert_ids = draw_expert_ids(jax.random.fold_in(jax.random.fold_in(key_list[14], part), 71), part)
    slots = draw_slots(jax.random.fold_in(jax.random.fold_in(key_list[14], part), 71), part)
    w_gate = normal_values(key_list[11], (D, EXPERTS * FFW), D ** -0.5, 0.0625, ((1, 16),))
    w_up = normal_values(key_list[12], (D, EXPERTS * FFW), D ** -0.5, 0.0625, ((1, 16),))
    w_down = normal_values(key_list[13], (EXPERTS * FFW, D), FFW ** -0.5, 0.1875, ((0, 16),))
    return dict(cache_kv=cache_kv, new_kv=new_kv, queries=queries, lengths=lengths, resid=resid, value_up=value_up, out_proj=out_proj, norm_gain=norm_gain, router=router, expert_ids=expert_ids, slots=slots, w_gate=w_gate, w_up=w_up, w_down=w_down)


route_scale = 2.827
norm_eps = 1e-06

def attend_one(packed):
    cache_rows, new_rows, query_rows, length = packed
    score_scale = 1.0 / QK ** 0.5
    query_full = query_rows.astype(jnp.float32)
    cache_full = cache_rows.astype(jnp.float32)
    new_full = new_rows.astype(jnp.float32)
    score_cache = jnp.einsum('shk,pk->shp', query_full, cache_full) * score_scale
    is_live = jnp.arange(CACHE, dtype=jnp.int32) < length
    score_cache = jnp.where(is_live[None, None, :], score_cache, -jnp.inf)
    score_new = jnp.einsum('shk,tk->sht', query_full, new_full) * score_scale
    step_ids = jnp.arange(STEPS, dtype=jnp.int32)
    causal = step_ids[None, :] <= step_ids[:, None]
    score_new = jnp.where(causal[:, None, :], score_new, -jnp.inf)
    row_peak = jnp.maximum(lax.optimization_barrier(jnp.max(score_cache, axis=-1)), lax.optimization_barrier(jnp.max(score_new, axis=-1)))
    exp_cache = jnp.exp(score_cache - row_peak[..., None])
    exp_new = jnp.exp(score_new - row_peak[..., None])
    exp_total = lax.optimization_barrier(jnp.sum(exp_cache, axis=-1)) + lax.optimization_barrier(jnp.sum(exp_new, axis=-1))
    prob_cache = (exp_cache / exp_total[..., None]).astype(jnp.bfloat16)
    prob_new = (exp_new / exp_total[..., None]).astype(jnp.bfloat16)
    context = jnp.einsum('shp,pc->shc', prob_cache.astype(jnp.float32), cache_full[:, :LAT])
    context = context + jnp.einsum('sht,tc->shc', prob_new.astype(jnp.float32), new_full[:, :LAT])
    return context.astype(jnp.bfloat16)

def reference(cache_kv, new_kv, queries, lengths, resid, value_up, out_proj, norm_gain, router, expert_ids, slots, w_gate, w_up, w_down):
    contexts = lax.map(attend_one, (cache_kv, new_kv, queries, lengths))
    values = jnp.einsum('bshc,chv->bshv', contexts.astype(jnp.float32), value_up.reshape(LAT, H, VH).astype(jnp.float32)).astype(jnp.bfloat16)
    rows_all = BATCH * STEPS
    attended = jnp.dot(values.reshape(rows_all, H * VH), out_proj, preferred_element_type=jnp.float32)
    hidden = resid.reshape(rows_all, D).astype(jnp.float32) + attended
    mean_square = lax.optimization_barrier(jnp.mean(hidden * hidden, axis=-1, keepdims=True))
    normed = (hidden * lax.rsqrt(mean_square + norm_eps) * norm_gain.astype(jnp.float32)).astype(jnp.bfloat16)
    logits = jnp.dot(normed, router, preferred_element_type=jnp.float32)
    route_ids = expert_ids.reshape(rows_all, TOP).astype(jnp.int32)
    route_slots = slots.reshape(rows_all, TOP).astype(jnp.int32)
    picked = jnp.take_along_axis(logits, route_ids, axis=1)
    gates = jax.nn.sigmoid(picked)
    weights = route_scale * gates / lax.optimization_barrier(jnp.sum(gates, axis=1, keepdims=True))
    is_kept = route_slots < CAP
    token_index = jnp.broadcast_to(jnp.arange(rows_all, dtype=jnp.int32)[:, None], (rows_all, TOP))
    source = token_index // TOK_DEV
    slot_total = EXPERTS * N_EP * CAP
    flat_slot = route_ids * (N_EP * CAP) + source * CAP + route_slots
    flat_slot = jnp.where(is_kept, flat_slot, slot_total).astype(jnp.int32)
    owner_row = jnp.full((slot_total + 1,), rows_all, dtype=jnp.int32).at[flat_slot.reshape(-1)].set(token_index.reshape(-1))
    share_row = jnp.zeros((slot_total + 1,), jnp.float32).at[flat_slot.reshape(-1)].set(weights.reshape(-1))
    owner_row = owner_row[:slot_total].reshape(EXPERTS, N_EP * CAP)
    share_row = share_row[:slot_total].reshape(EXPERTS, N_EP * CAP)
    padded = jnp.concatenate([normed, jnp.zeros((1, D), jnp.bfloat16)], axis=0)

    def expert_step(expert_mix, packed):
        expert_index, owners, shares = packed
        token_rows = padded[owners]
        gate_cols = lax.dynamic_slice_in_dim(w_gate, expert_index * FFW, FFW, 1)
        up_cols = lax.dynamic_slice_in_dim(w_up, expert_index * FFW, FFW, 1)
        down_rows = lax.dynamic_slice_in_dim(w_down, expert_index * FFW, FFW, 0)
        gate = jnp.dot(token_rows, gate_cols, preferred_element_type=jnp.float32)
        upward = jnp.dot(token_rows, up_cols, preferred_element_type=jnp.float32)
        act = (jax.nn.silu(gate) * upward).astype(jnp.bfloat16)
        produced = jnp.dot(act, down_rows, preferred_element_type=jnp.float32) * shares[:, None]
        return (expert_mix.at[owners].add(produced), None)
    start_mix = jnp.zeros((rows_all + 1, D), jnp.float32)
    expert_mix, _ = lax.scan(expert_step, start_mix, (jnp.arange(EXPERTS, dtype=jnp.int32), owner_row, share_row))
    mixed = (hidden + expert_mix[:rows_all]).astype(jnp.bfloat16)
    return mixed.reshape(BATCH, STEPS, D)
```

```python
import functools
import math

import jax
import jax.numpy as jnp
from jax import lax
from jax.experimental import pallas as pl
from jax.experimental.pallas import tpu as pltpu
from jax.sharding import PartitionSpec as P

D = 7168
H = 64
LAT = 512
VH = 128
EXPERTS = 16
TOP = 8
CAP = 2
QK = 192


route_scale = 2.827
norm_eps = 1e-06


def softmax_parts(score_cache, score_new):
    row_peak = jnp.maximum(jnp.max(score_cache, axis=-1), jnp.max(score_new, axis=-1))
    exp_cache = jnp.exp(score_cache - row_peak[..., None])
    exp_new = jnp.exp(score_new - row_peak[..., None])
    exp_total = jnp.sum(exp_cache, axis=-1) + jnp.sum(exp_new, axis=-1)
    prob_cache = (exp_cache / exp_total[..., None]).astype(jnp.bfloat16)
    prob_new = (exp_new / exp_total[..., None]).astype(jnp.bfloat16)
    return (prob_cache, prob_new)


def attention(cache_kv, new_kv, queries, lengths):
    score_scale = 1.0 / math.sqrt(QK)
    cache_len = cache_kv.shape[1]
    step_count = new_kv.shape[1]
    score_new = (
        jnp.einsum("bshk,btk->bsht", queries, new_kv, preferred_element_type=jnp.float32)
        * score_scale
    )
    step_ids = jnp.arange(step_count, dtype=jnp.int32)
    causal = step_ids[None, :] <= step_ids[:, None]
    score_new = jnp.where(causal[None, :, None, :], score_new, -jnp.inf)
    score_cache = (
        jnp.einsum("bshk,bpk->bshp", queries, cache_kv, preferred_element_type=jnp.float32)
        * score_scale
    )
    position = jnp.arange(cache_len, dtype=jnp.int32)
    is_live = position[None, :] < lengths[:, None]
    score_cache = jnp.where(is_live[:, None, None, :], score_cache, -jnp.inf)
    prob_cache, prob_new = softmax_parts(score_cache, score_new)
    context = jnp.einsum(
        "bshp,bpc->bshc", prob_cache, cache_kv[:, :, :LAT], preferred_element_type=jnp.float32
    )
    context = context + jnp.einsum(
        "bsht,btc->bshc", prob_new, new_kv[:, :, :LAT], preferred_element_type=jnp.float32
    )
    return context.astype(jnp.bfloat16)


F32 = jnp.float32
BF16 = jnp.bfloat16
CORES = 2
LINE = 4
CHUNKS = 4


def loop(count, step, start=0):
    lax.fori_loop(start, count, lambda i, carry: (step(i), carry)[1], 0)


def layer_kernel(
    n,
    ctx_ref,
    resid_ref,
    gain_ref,
    router_ref,
    ids_ref,
    slots_ref,
    vu_hbm,
    op_hbm,
    wg_hbm,
    wu_hbm,
    wd_hbm,
    out_ref,
    vu,
    op,
    wg,
    wu,
    wd,
    ctx_in,
    rows32,
    acc32,
    gate_acc,
    up_acc,
    hid,
    part,
    pair_sum,
    line_sum,
    in_core0,
    in_mid0,
    in_line0,
    in_core1,
    in_mid1,
    in_line1,
    gathered,
    share_out,
    share_in,
    share_all,
    w_sem,
    ctx_send,
    ctx_recv,
    share_send,
    share_recv,
    core_sem,
    mid_send,
    mid_recv,
    line_send,
    line_recv,
):
    me = lax.axis_index("ep")
    mids = n // (CORES * LINE)
    c = me % CORES
    b = (me // CORES) % mids
    a = me // (CORES * mids)
    toks, width = resid_ref.shape
    part_w = width // CHUNKS
    rows_each = ctx_ref.shape[1]
    heads_per = rows_each // toks
    value_cols = vu.shape[1]
    total = n * toks
    fan = CORES * mids
    per = 8 // toks

    def stack(ref, block, rows):
        group = 8 // rows

        def put(g):
            tile = jnp.concatenate([block(g * group + h) for h in range(group)], axis=0)
            ref[pl.ds(pl.multiple_of(g * 8, 8), 8), :] = tile

        loop(n // group, put)

    def dev(aa, bb, cc):
        return (aa * mids + bb) * CORES + cc

    def send(src, dst, s_sem, r_sem, target):
        return pltpu.make_async_remote_copy(
            src_ref=src,
            dst_ref=dst,
            send_sem=s_sem,
            recv_sem=r_sem,
            device_id={"ep": target},
            device_id_type=pl.DeviceIdType.MESH,
        )

    def cols(ch):
        return pl.ds(pl.multiple_of(ch * part_w, part_w), part_w)

    def op_copy(ch):
        return pltpu.make_async_copy(op_hbm.at[:, cols(ch)], op.at[ch], w_sem.at[0, ch])

    def wg_copy(ch):
        return pltpu.make_async_copy(wg_hbm.at[cols(ch), :], wg.at[ch], w_sem.at[1, ch])

    def wu_copy(ch):
        return pltpu.make_async_copy(wu_hbm.at[cols(ch), :], wu.at[ch], w_sem.at[2, ch])

    def wd_copy(ch):
        return pltpu.make_async_copy(wd_hbm.at[:, cols(ch)], wd.at[ch], w_sem.at[3, ch])

    vu_copy = pltpu.make_async_copy(vu_hbm, vu, w_sem.at[4, 0])
    vu_copy.start()

    barrier = pltpu.get_barrier_semaphore()

    def greet(i):
        pl.semaphore_signal(
            barrier,
            inc=1,
            device_id={"ep": (me + i) % n},
            device_id_type=pl.DeviceIdType.MESH,
        )

    loop(n, greet, 1)
    loop(CHUNKS, lambda ch: op_copy(ch).start())
    pl.semaphore_wait(barrier, n - 1)

    def ctx_copy(i):
        to = (me + i) % n
        return send(ctx_ref.at[to], ctx_in.at[me], ctx_send.at[to], ctx_recv.at[me], to)

    def ctx_arrival(i):
        frm = (me + i) % n
        return send(ctx_ref.at[frm], ctx_in.at[frm], ctx_send.at[frm], ctx_recv.at[frm], frm)

    loop(n, lambda i: ctx_copy(i).start(), 1)

    def start_ffn(ch):
        wg_copy(ch).start()
        wu_copy(ch).start()

    loop(CHUNKS, start_ffn)
    loop(CHUNKS, lambda ch: wd_copy(ch).start())

    lane = lax.broadcasted_iota(jnp.int32, (toks, EXPERTS), 1)
    named = jnp.zeros((toks, EXPERTS), F32)
    kept = jnp.zeros((toks, EXPERTS), F32)
    for k in range(TOP):
        hit = jnp.where(ids_ref[:, k : k + 1] == lane, 1.0, 0.0)
        named = named + hit
        kept = kept + jnp.where(slots_ref[:, k : k + 1] < CAP, hit, 0.0)

    ctx_in[me] = ctx_ref[me]
    vu_copy.wait()
    loop(n, lambda i: ctx_arrival(i).wait_recv(), 1)

    if rows_each % 16 == 0:
        head_rows = ctx_in[...].reshape(n * rows_each, LAT)
    else:

        stack(rows32, lambda i: ctx_in[i].astype(F32), rows_each)
        head_rows = rows32[...].astype(BF16)
    values = jnp.dot(head_rows, vu[...], preferred_element_type=F32)
    if heads_per > 1:
        shape = (n * rows_each, value_cols)
        row_head = lax.broadcasted_iota(jnp.int32, shape, 0) % heads_per
        col_head = lax.broadcasted_iota(jnp.int32, shape, 1) // (value_cols // heads_per)
        values = jnp.where(row_head == col_head, values, 0.0).astype(BF16)
        shape = (total, n * rows_each)
        row_tok = lax.broadcasted_iota(jnp.int32, shape, 1) // heads_per
        fold = jnp.where(row_tok == lax.broadcasted_iota(jnp.int32, shape, 0), 1.0, 0.0)
        values = jnp.dot(fold.astype(BF16), values, preferred_element_type=F32)
    values = values.astype(BF16)

    def reduce_scatter(which, produce, finish):
        in_core, in_mid, in_line = (
            (in_core0, in_mid0, in_line0) if which == 0 else (in_core1, in_mid1, in_line1)
        )

        def core_copy(ch):
            return send(
                part.at[ch, 1 - c],
                in_core.at[ch],
                core_sem.at[which, 0, ch],
                core_sem.at[which, 1, ch],
                dev(a, b, 1 - c),
            )

        def mid_copy(ch, i):
            bb = (b + i) % mids
            return send(
                pair_sum.at[ch, bb],
                in_mid.at[ch, b],
                mid_send.at[which, ch, bb],
                mid_recv.at[which, ch, b],
                dev(a, bb, c),
            )

        def mid_arrival(ch, bb):
            return send(
                pair_sum.at[ch, bb],
                in_mid.at[ch, bb],
                mid_send.at[which, ch, bb],
                mid_recv.at[which, ch, bb],
                dev(a, bb, c),
            )

        def line_copy(ch, i):
            aa = (a + i) % LINE
            return send(
                line_sum.at[ch, aa],
                in_line.at[ch, a],
                line_send.at[which, ch, aa],
                line_recv.at[which, ch, a],
                dev(aa, b, c),
            )

        def line_arrival(ch, aa):
            return send(
                line_sum.at[ch, aa],
                in_line.at[ch, aa],
                line_send.at[which, ch, aa],
                line_recv.at[which, ch, aa],
                dev(aa, b, c),
            )

        def stage1(ch):
            acc32[...] = produce(ch)

            def spread(g):
                tile = acc32[pl.ds(pl.multiple_of(g * 8, 8), 8), :]
                for h in range(per):
                    d = g * per + h
                    part[ch, d % CORES, (d // CORES) % mids, d // fan] = tile[
                        h * toks : (h + 1) * toks
                    ].astype(BF16)

            loop(n // per, spread)
            core_copy(ch).start()

        def stage2(ch):
            core_copy(ch).wait_recv()

            def add_pair(k):
                bb, aa = k // LINE, k % LINE
                pair_sum[ch, bb, aa] = (
                    part[ch, c, bb, aa].astype(F32) + in_core[ch, bb, aa].astype(F32)
                ).astype(BF16)

            loop(mids * LINE, add_pair)
            loop(mids, lambda i: mid_copy(ch, i).start(), 1)

        def stage3(ch):
            loop(mids, lambda i: mid_arrival(ch, (b + i) % mids).wait_recv(), 1)

            def add_mid(aa):
                acc = pair_sum[ch, b, aa].astype(F32)
                acc = lax.fori_loop(
                    1, mids, lambda i, t: t + in_mid[ch, (b + i) % mids, aa].astype(F32), acc
                )
                line_sum[ch, aa] = acc.astype(BF16)

            loop(LINE, add_mid)
            loop(LINE, lambda i: line_copy(ch, i).start(), 1)

        def stage4(ch):
            acc = line_sum[ch, a].astype(F32)
            for i in range(1, LINE):
                aa = (a + i) % LINE
                line_arrival(ch, aa).wait_recv()
                acc = acc + in_line[ch, aa].astype(F32)
            finish(ch, acc)

        def step(t):
            for delay, stage in enumerate((stage1, stage2, stage3, stage4)):
                pl.when((t >= delay) & (t < CHUNKS + delay))(
                    functools.partial(stage, t - delay)
                )

        loop(CHUNKS + 3, step)

        def drain(ch):
            core_copy(ch).wait_send()
            loop(mids, lambda i: mid_copy(ch, i).wait_send(), 1)
            loop(LINE, lambda i: line_copy(ch, i).wait_send(), 1)

        loop(CHUNKS, drain)

    def attended_part(ch):
        op_copy(ch).wait()
        return jnp.dot(values, op[ch], preferred_element_type=F32)

    def keep_hidden(ch, acc):
        hid[ch] = acc + resid_ref[:, cols(ch)].astype(F32)

    reduce_scatter(0, attended_part, keep_hidden)

    square = jnp.zeros((toks, 1), F32)
    for ch in range(CHUNKS):
        square = square + jnp.sum(hid[ch] * hid[ch], axis=-1, keepdims=True)
    scale = lax.rsqrt(square / width + norm_eps)

    def leg_line(ch, i):
        aa = (a + i) % LINE
        blk = gathered.at[ch, c, b, a]
        return send(blk, blk, line_send.at[2, ch, aa], line_recv.at[2, ch, a], dev(aa, b, c))

    def leg_line_arrival(ch, aa):
        blk = gathered.at[ch, c, b, aa]
        return send(blk, blk, line_send.at[2, ch, aa], line_recv.at[2, ch, aa], dev(aa, b, c))

    def leg_mid(ch, i):
        bb = (b + i) % mids
        blk = gathered.at[ch, c, b]
        return send(blk, blk, mid_send.at[2, ch, bb], mid_recv.at[2, ch, b], dev(a, bb, c))

    def leg_mid_arrival(ch, bb):
        blk = gathered.at[ch, c, bb]
        return send(blk, blk, mid_send.at[2, ch, bb], mid_recv.at[2, ch, bb], dev(a, bb, c))

    def leg_core(ch):
        blk = gathered.at[ch, c]
        return send(
            blk, blk, core_sem.at[2, 0, ch], core_sem.at[2, 1, ch], dev(a, b, 1 - c)
        )

    def leg_core_arrival(ch):
        blk = gathered.at[ch, 1 - c]
        return send(
            blk, blk, core_sem.at[2, 0, ch], core_sem.at[2, 1, ch], dev(a, b, 1 - c)
        )

    logits = jnp.zeros((toks, EXPERTS), F32)
    for ch in range(CHUNKS):
        span = slice(ch * part_w, (ch + 1) * part_w)
        normed = (hid[ch] * scale * gain_ref[:, span].astype(F32)).astype(BF16)
        gathered[ch, c, b, a] = normed
        for i in range(1, LINE):
            leg_line(ch, i).start()
        logits = logits + lax.dot_general(
            normed,
            router_ref[:, span],
            (((1,), (1,)), ((), ())),
            preferred_element_type=F32,
        )
    gates = jax.nn.sigmoid(logits)
    shares = route_scale * gates / jnp.sum(gates * named, axis=1, keepdims=True) * kept
    share_out[...] = jnp.zeros_like(share_out)
    share_out[:, :EXPERTS] = shares

    def share_copy(i):
        to = (me + i) % n
        return send(share_out, share_in.at[me], share_send.at[to], share_recv.at[me], to)

    def share_arrival(i):
        frm = (me + i) % n
        return send(share_out, share_in.at[frm], share_send.at[frm], share_recv.at[frm], frm)

    gate_acc[...] = jnp.zeros_like(gate_acc)
    up_acc[...] = jnp.zeros_like(up_acc)

    def hop_mid(ch):
        for i in range(1, LINE):
            leg_line_arrival(ch, (a + i) % LINE).wait_recv()
        loop(mids, lambda i: leg_mid(ch, i).start(), 1)

    def hop_core(ch):
        loop(mids, lambda i: leg_mid_arrival(ch, (b + i) % mids).wait_recv(), 1)
        leg_core(ch).start()

    def multiply(ch):
        leg_core_arrival(ch).wait_recv()

        def block(d):
            return gathered[ch, d % CORES, (d // CORES) % mids, d // fan].astype(F32)

        stack(acc32, block, toks)
        x = acc32[...].astype(BF16)
        wg_copy(ch).wait()
        gate_acc[...] += jnp.dot(x, wg[ch], preferred_element_type=F32)
        wu_copy(ch).wait()
        up_acc[...] += jnp.dot(x, wu[ch], preferred_element_type=F32)

    def gather_step(t):
        for delay, stage in enumerate((hop_mid, hop_core, multiply)):
            pl.when((t >= delay) & (t < CHUNKS + delay))(functools.partial(stage, t - delay))

    loop(n, lambda i: share_copy(i).start(), 1)
    loop(CHUNKS + 2, gather_step)

    share_in[me] = share_out[...]
    loop(n, lambda i: share_arrival(i).wait_recv(), 1)

    stack(share_all, lambda d: share_in[d], toks)
    mine = lax.broadcasted_iota(jnp.int32, share_all.shape, 1) == me // (n // EXPERTS)
    share = jnp.sum(jnp.where(mine, share_all[...], 0.0), axis=1, keepdims=True)
    gate = gate_acc[...]
    act = (gate * jax.nn.sigmoid(gate) * up_acc[...]).astype(BF16)

    def expert_part(ch):
        wd_copy(ch).wait()
        return jnp.dot(act, wd[ch], preferred_element_type=F32) * share

    def put_out(ch, acc):
        out_ref[:, cols(ch)] = (hid[ch] + acc).astype(BF16)

    reduce_scatter(1, expert_part, put_out)

    def drain_pairs(i):
        ctx_copy(i).wait_send()
        share_copy(i).wait_send()

    loop(n, drain_pairs, 1)

    def drain_gather(ch):
        for i in range(1, LINE):
            leg_line(ch, i).wait_send()
        loop(mids, lambda i: leg_mid(ch, i).wait_send(), 1)
        leg_core(ch).wait_send()

    loop(CHUNKS, drain_gather)


def body(
    cache_kv,
    new_kv,
    queries,
    lengths,
    resid,
    value_up,
    out_proj,
    norm_gain,
    router,
    expert_ids,
    slots,
    w_gate,
    w_up,
    w_down,
):
    n = lax.axis_size("ep")
    context = attention(cache_kv, new_kv, queries, lengths)
    toks = context.shape[0] * context.shape[1]
    heads = context.shape[2]
    width = resid.shape[-1]
    context = context.reshape(toks, heads, LAT)
    value_cols = value_up.shape[1]
    heads_per = max(1, value_cols // VH)
    if value_cols < VH:
        context = jnp.repeat(context, VH // value_cols, axis=1)
    outgoing = context.reshape(toks, n, heads_per, LAT).transpose(1, 0, 2, 3)
    outgoing = outgoing.reshape(n, toks * heads_per, LAT)
    hidden_units = w_gate.shape[1]
    mids = n // (CORES * LINE)
    part_w = width // CHUNKS
    total = n * toks
    vmem = pl.BlockSpec(memory_space=pltpu.VMEM)
    hbm = pl.BlockSpec(memory_space=pl.ANY)
    landing = [
        pltpu.VMEM((CHUNKS, mids, LINE, toks, part_w), BF16),
        pltpu.VMEM((CHUNKS, mids, LINE, toks, part_w), BF16),
        pltpu.VMEM((CHUNKS, LINE, toks, part_w), BF16),
    ]
    dma = pltpu.SemaphoreType.DMA
    mixed = pl.pallas_call(
        functools.partial(layer_kernel, n),
        out_shape=jax.ShapeDtypeStruct((toks, width), BF16),
        in_specs=[vmem] * 6 + [hbm] * 5,
        out_specs=vmem,
        scratch_shapes=[
            pltpu.VMEM(value_up.shape, BF16),
            pltpu.VMEM((CHUNKS, out_proj.shape[0], part_w), BF16),
            pltpu.VMEM((CHUNKS, part_w, hidden_units), BF16),
            pltpu.VMEM((CHUNKS, part_w, hidden_units), BF16),
            pltpu.VMEM((CHUNKS, hidden_units, part_w), BF16),
            pltpu.VMEM(outgoing.shape, BF16),
            pltpu.VMEM((n * toks * heads_per if toks * heads_per % 16 else 8, LAT), F32),
            pltpu.VMEM((total, part_w), F32),
            pltpu.VMEM((total, hidden_units), F32),
            pltpu.VMEM((total, hidden_units), F32),
            pltpu.VMEM((CHUNKS, toks, part_w), F32),
            pltpu.VMEM((CHUNKS, CORES, mids, LINE, toks, part_w), BF16),
            pltpu.VMEM((CHUNKS, mids, LINE, toks, part_w), BF16),
            pltpu.VMEM((CHUNKS, LINE, toks, part_w), BF16),
            *landing,
            *landing,
            pltpu.VMEM((CHUNKS, CORES, mids, LINE, toks, part_w), BF16),
            pltpu.VMEM((toks, 128), F32),
            pltpu.VMEM((n, toks, 128), F32),
            pltpu.VMEM((total, 128), F32),
            dma((5, CHUNKS)),
            dma((n,)),
            dma((n,)),
            dma((n,)),
            dma((n,)),
            dma((3, 2, CHUNKS)),
            dma((3, CHUNKS, mids)),
            dma((3, CHUNKS, mids)),
            dma((3, CHUNKS, LINE)),
            dma((3, CHUNKS, LINE)),
        ],
        compiler_params=pltpu.CompilerParams(
            collective_id=0, has_side_effects=True, vmem_limit_bytes=67043328
        ),
    )(
        outgoing,
        resid.reshape(toks, width),
        norm_gain.reshape(1, width),
        router.T,
        expert_ids.reshape(toks, TOP),
        slots.reshape(toks, TOP),
        value_up,
        out_proj,
        w_gate,
        w_up,
        w_down,
    )
    return mixed.reshape(resid.shape)


def solution(mesh):
    return jax.shard_map(
        body,
        mesh=mesh,
        in_specs=(
            P(("rep", "ep"), None, None),
            P(("rep", "ep"), None, None),
            P(("rep", "ep"), None, None, None),
            P(("rep", "ep")),
            P(("rep", "ep"), None, None),
            P(None, "ep"),
            P("ep", None),
            P(),
            P(),
            P(("rep", "ep"), None, None),
            P(("rep", "ep"), None, None),
            P(None, "ep"),
            P(None, "ep"),
            P("ep", None),
        ),
        out_specs=P(("rep", "ep"), None, None),
        check_vma=False,
    )
```

```python
import functools
import math

import jax
import jax.numpy as jnp
from jax import lax
from jax.experimental import pallas as pl
from jax.experimental.pallas import tpu as pltpu
from jax.sharding import PartitionSpec as P

D = 7168
H = 64
LAT = 512
VH = 128
EXPERTS = 16
TOP = 8
CAP = 2
QK = 192


route_scale = 2.827
norm_eps = 1e-06


F32 = jnp.float32
BF16 = jnp.bfloat16
CORES = 2
LINE = 4
CHUNKS = 4


def loop(count, step, start=0):
    lax.fori_loop(start, count, lambda i, carry: (step(i), carry)[1], 0)


def layer_kernel(
    n,
    len_ref,
    new_ref,
    gain_ref,
    router_ref,
    ids_ref,
    slots_ref,
    cache_hbm,
    query_hbm,
    resid_hbm,
    vu_hbm,
    op_hbm,
    wg_hbm,
    wu_hbm,
    wd_hbm,
    out_ref,
    vu,
    op,
    wg,
    wu,
    wd,
    keys,
    fresh,
    query,
    resid,
    ctx32,
    ctx_ref,
    ctx_in,
    rows32,
    acc32,
    gate_acc,
    up_acc,
    hid,
    part,
    pair_sum,
    line_sum,
    in_core0,
    in_mid0,
    in_line0,
    in_core1,
    in_mid1,
    in_line1,
    gathered,
    share_out,
    share_in,
    share_all,
    w_sem,
    key_sem,
    ctx_send,
    ctx_recv,
    share_send,
    share_recv,
    core_sem,
    mid_send,
    mid_recv,
    line_send,
    line_recv,
):
    me = lax.axis_index("ep")
    mids = n // (CORES * LINE)
    c = me % CORES
    b = (me // CORES) % mids
    a = me // (CORES * mids)
    seqs, steps, width = resid.shape
    toks = seqs * steps
    part_w = width // CHUNKS
    rows_each = ctx_ref.shape[1]
    heads_per = rows_each // toks
    value_cols = vu.shape[1]
    total = n * toks
    fan = CORES * mids
    per = 8 // toks

    def stack(ref, block, rows):
        group = 8 // rows

        def put(g):
            tile = jnp.concatenate([block(g * group + h) for h in range(group)], axis=0)
            ref[pl.ds(pl.multiple_of(g * 8, 8), 8), :] = tile

        loop(n // group, put)

    def dev(aa, bb, cc):
        return (aa * mids + bb) * CORES + cc

    def send(src, dst, s_sem, r_sem, target):
        return pltpu.make_async_remote_copy(
            src_ref=src,
            dst_ref=dst,
            send_sem=s_sem,
            recv_sem=r_sem,
            device_id={"ep": target},
            device_id_type=pl.DeviceIdType.MESH,
        )

    def cols(ch):
        return pl.ds(pl.multiple_of(ch * part_w, part_w), part_w)

    def op_copy(ch):
        return pltpu.make_async_copy(op_hbm.at[:, cols(ch)], op.at[ch], w_sem.at[0, ch])

    def wg_copy(ch):
        return pltpu.make_async_copy(wg_hbm.at[cols(ch), :], wg.at[ch], w_sem.at[1, ch])

    def wu_copy(ch):
        return pltpu.make_async_copy(wu_hbm.at[cols(ch), :], wu.at[ch], w_sem.at[2, ch])

    def wd_copy(ch):
        return pltpu.make_async_copy(wd_hbm.at[:, cols(ch)], wd.at[ch], w_sem.at[3, ch])

    vu_copy = pltpu.make_async_copy(vu_hbm, vu, w_sem.at[4, 0])
    resid_copy = pltpu.make_async_copy(resid_hbm, resid, w_sem.at[4, 1])
    cache_len = cache_hbm.shape[2]

    def key_copy(q):
        return pltpu.make_async_copy(cache_hbm.at[q], keys.at[q], key_sem.at[0, q])

    def query_copy(q):
        return pltpu.make_async_copy(query_hbm.at[q], query.at[q], key_sem.at[1, q])

    for q in range(seqs):
        query_copy(q).start()
        key_copy(q).start()
    vu_copy.start()
    resid_copy.start()

    barrier = pltpu.get_barrier_semaphore()

    def greet(i):
        pl.semaphore_signal(
            barrier,
            inc=1,
            device_id={"ep": (me + i) % n},
            device_id_type=pl.DeviceIdType.MESH,
        )

    loop(n, greet, 1)
    loop(CHUNKS, lambda ch: op_copy(ch).start())

    def start_ffn(ch):
        wg_copy(ch).start()
        wu_copy(ch).start()

    loop(CHUNKS, start_ffn)
    loop(CHUNKS, lambda ch: wd_copy(ch).start())

    rows_q, span_new = query.shape[1], fresh.shape[1]
    heads = rows_q // steps
    score_scale = 1.0 / math.sqrt(QK)
    fresh[...] = jnp.zeros_like(fresh)
    for q in range(seqs):
        fresh[q, :steps, :] = new_ref[q]
    place = lax.broadcasted_iota(jnp.int32, (rows_q, cache_len), 1)
    newer = lax.broadcasted_iota(jnp.int32, (rows_q, span_new), 1) <= (
        lax.broadcasted_iota(jnp.int32, (rows_q, span_new), 0) // heads
    )
    for q in range(seqs):
        query_copy(q).wait()
        key_copy(q).wait()
        old = jnp.dot(query[q], keys[q], preferred_element_type=F32) * score_scale
        old = jnp.where(place < len_ref[q], old, -jnp.inf)
        new = lax.dot_general(
            query[q], fresh[q], (((1,), (1,)), ((), ())), preferred_element_type=F32
        )
        new = jnp.where(newer, new * score_scale, -jnp.inf)
        peak = jnp.maximum(
            jnp.max(old, axis=-1, keepdims=True), jnp.max(new, axis=-1, keepdims=True)
        )
        old = jnp.exp(old - peak)
        new = jnp.exp(new - peak)
        inverse = 1.0 / (
            jnp.sum(old, axis=-1, keepdims=True) + jnp.sum(new, axis=-1, keepdims=True)
        )
        ctx32[q] = lax.dot_general(
            (old * inverse).astype(BF16),
            keys[q, :LAT, :],
            (((1,), (1,)), ((), ())),
            preferred_element_type=F32,
        ) + jnp.dot(
            (new * inverse).astype(BF16), fresh[q, :, :LAT], preferred_element_type=F32
        )
    for j in range(n):
        first = (j * value_cols) // VH
        rows = [
            ctx32[q, t * heads + first : t * heads + first + heads_per, :]
            for q in range(seqs)
            for t in range(steps)
        ]
        ctx_ref[j] = jnp.concatenate(rows, axis=0).astype(BF16)
    pl.semaphore_wait(barrier, n - 1)

    def ctx_copy(i):
        to = (me + i) % n
        return send(ctx_ref.at[to], ctx_in.at[me], ctx_send.at[to], ctx_recv.at[me], to)

    def ctx_arrival(i):
        frm = (me + i) % n
        return send(ctx_ref.at[frm], ctx_in.at[frm], ctx_send.at[frm], ctx_recv.at[frm], frm)

    loop(n, lambda i: ctx_copy(i).start(), 1)

    lane = lax.broadcasted_iota(jnp.int32, (toks, EXPERTS), 1)
    named = jnp.zeros((toks, EXPERTS), F32)
    kept = jnp.zeros((toks, EXPERTS), F32)
    for k in range(TOP):
        hit = jnp.where(ids_ref[:, k : k + 1] == lane, 1.0, 0.0)
        named = named + hit
        kept = kept + jnp.where(slots_ref[:, k : k + 1] < CAP, hit, 0.0)

    ctx_in[me] = ctx_ref[me]
    vu_copy.wait()
    loop(n, lambda i: ctx_arrival(i).wait_recv(), 1)

    if rows_each % 16 == 0:
        head_rows = ctx_in[...].reshape(n * rows_each, LAT)
    else:

        stack(rows32, lambda i: ctx_in[i].astype(F32), rows_each)
        head_rows = rows32[...].astype(BF16)
    values = jnp.dot(head_rows, vu[...], preferred_element_type=F32)
    if heads_per > 1:
        shape = (n * rows_each, value_cols)
        row_head = lax.broadcasted_iota(jnp.int32, shape, 0) % heads_per
        col_head = lax.broadcasted_iota(jnp.int32, shape, 1) // (value_cols // heads_per)
        values = jnp.where(row_head == col_head, values, 0.0).astype(BF16)
        shape = (total, n * rows_each)
        row_tok = lax.broadcasted_iota(jnp.int32, shape, 1) // heads_per
        fold = jnp.where(row_tok == lax.broadcasted_iota(jnp.int32, shape, 0), 1.0, 0.0)
        values = jnp.dot(fold.astype(BF16), values, preferred_element_type=F32)
    values = values.astype(BF16)

    def reduce_scatter(which, produce, finish):
        in_core, in_mid, in_line = (
            (in_core0, in_mid0, in_line0) if which == 0 else (in_core1, in_mid1, in_line1)
        )

        def core_copy(ch):
            return send(
                part.at[ch, 1 - c],
                in_core.at[ch],
                core_sem.at[which, 0, ch],
                core_sem.at[which, 1, ch],
                dev(a, b, 1 - c),
            )

        def mid_copy(ch, i):
            bb = (b + i) % mids
            return send(
                pair_sum.at[ch, bb],
                in_mid.at[ch, b],
                mid_send.at[which, ch, bb],
                mid_recv.at[which, ch, b],
                dev(a, bb, c),
            )

        def mid_arrival(ch, bb):
            return send(
                pair_sum.at[ch, bb],
                in_mid.at[ch, bb],
                mid_send.at[which, ch, bb],
                mid_recv.at[which, ch, bb],
                dev(a, bb, c),
            )

        def line_copy(ch, i):
            aa = (a + i) % LINE
            return send(
                line_sum.at[ch, aa],
                in_line.at[ch, a],
                line_send.at[which, ch, aa],
                line_recv.at[which, ch, a],
                dev(aa, b, c),
            )

        def line_arrival(ch, aa):
            return send(
                line_sum.at[ch, aa],
                in_line.at[ch, aa],
                line_send.at[which, ch, aa],
                line_recv.at[which, ch, aa],
                dev(aa, b, c),
            )

        def stage1(ch):
            acc32[...] = produce(ch)

            def spread(g):
                tile = acc32[pl.ds(pl.multiple_of(g * 8, 8), 8), :]
                for h in range(per):
                    d = g * per + h
                    part[ch, d % CORES, (d // CORES) % mids, d // fan] = tile[
                        h * toks : (h + 1) * toks
                    ].astype(BF16)

            loop(n // per, spread)
            core_copy(ch).start()

        def stage2(ch):
            core_copy(ch).wait_recv()

            def add_pair(k):
                bb, aa = k // LINE, k % LINE
                pair_sum[ch, bb, aa] = (
                    part[ch, c, bb, aa].astype(F32) + in_core[ch, bb, aa].astype(F32)
                ).astype(BF16)

            loop(mids * LINE, add_pair)
            loop(mids, lambda i: mid_copy(ch, i).start(), 1)

        def stage3(ch):
            loop(mids, lambda i: mid_arrival(ch, (b + i) % mids).wait_recv(), 1)

            def add_mid(aa):
                acc = pair_sum[ch, b, aa].astype(F32)
                acc = lax.fori_loop(
                    1, mids, lambda i, t: t + in_mid[ch, (b + i) % mids, aa].astype(F32), acc
                )
                line_sum[ch, aa] = acc.astype(BF16)

            loop(LINE, add_mid)
            loop(LINE, lambda i: line_copy(ch, i).start(), 1)

        def stage4(ch):
            acc = line_sum[ch, a].astype(F32)
            for i in range(1, LINE):
                aa = (a + i) % LINE
                line_arrival(ch, aa).wait_recv()
                acc = acc + in_line[ch, aa].astype(F32)
            finish(ch, acc)

        def step(t):
            for delay, stage in enumerate((stage1, stage2, stage3, stage4)):
                pl.when((t >= delay) & (t < CHUNKS + delay))(
                    functools.partial(stage, t - delay)
                )

        loop(CHUNKS + 3, step)

        def drain(ch):
            core_copy(ch).wait_send()
            loop(mids, lambda i: mid_copy(ch, i).wait_send(), 1)
            loop(LINE, lambda i: line_copy(ch, i).wait_send(), 1)

        loop(CHUNKS, drain)

    def attended_part(ch):
        op_copy(ch).wait()
        return jnp.dot(values, op[ch], preferred_element_type=F32)

    def keep_hidden(ch, acc):
        rows = [resid[q, :, cols(ch)].astype(F32) for q in range(seqs)]
        hid[ch] = acc + jnp.concatenate(rows, axis=0)

    resid_copy.wait()
    reduce_scatter(0, attended_part, keep_hidden)

    square = jnp.zeros((toks, 1), F32)
    for ch in range(CHUNKS):
        square = square + jnp.sum(hid[ch] * hid[ch], axis=-1, keepdims=True)
    scale = lax.rsqrt(square / width + norm_eps)

    def leg_line(ch, i):
        aa = (a + i) % LINE
        blk = gathered.at[ch, c, b, a]
        return send(blk, blk, line_send.at[2, ch, aa], line_recv.at[2, ch, a], dev(aa, b, c))

    def leg_line_arrival(ch, aa):
        blk = gathered.at[ch, c, b, aa]
        return send(blk, blk, line_send.at[2, ch, aa], line_recv.at[2, ch, aa], dev(aa, b, c))

    def leg_mid(ch, i):
        bb = (b + i) % mids
        blk = gathered.at[ch, c, b]
        return send(blk, blk, mid_send.at[2, ch, bb], mid_recv.at[2, ch, b], dev(a, bb, c))

    def leg_mid_arrival(ch, bb):
        blk = gathered.at[ch, c, bb]
        return send(blk, blk, mid_send.at[2, ch, bb], mid_recv.at[2, ch, bb], dev(a, bb, c))

    def leg_core(ch):
        blk = gathered.at[ch, c]
        return send(
            blk, blk, core_sem.at[2, 0, ch], core_sem.at[2, 1, ch], dev(a, b, 1 - c)
        )

    def leg_core_arrival(ch):
        blk = gathered.at[ch, 1 - c]
        return send(
            blk, blk, core_sem.at[2, 0, ch], core_sem.at[2, 1, ch], dev(a, b, 1 - c)
        )

    logits = jnp.zeros((toks, EXPERTS), F32)
    for ch in range(CHUNKS):
        span = slice(ch * part_w, (ch + 1) * part_w)
        normed = (hid[ch] * scale * gain_ref[:, span].astype(F32)).astype(BF16)
        gathered[ch, c, b, a] = normed
        for i in range(1, LINE):
            leg_line(ch, i).start()
        logits = logits + lax.dot_general(
            normed,
            router_ref[:, span],
            (((1,), (1,)), ((), ())),
            preferred_element_type=F32,
        )
    gates = jax.nn.sigmoid(logits)
    shares = route_scale * gates / jnp.sum(gates * named, axis=1, keepdims=True) * kept
    share_out[...] = jnp.zeros_like(share_out)
    share_out[:, :EXPERTS] = shares

    def share_copy(i):
        to = (me + i) % n
        return send(share_out, share_in.at[me], share_send.at[to], share_recv.at[me], to)

    def share_arrival(i):
        frm = (me + i) % n
        return send(share_out, share_in.at[frm], share_send.at[frm], share_recv.at[frm], frm)

    gate_acc[...] = jnp.zeros_like(gate_acc)
    up_acc[...] = jnp.zeros_like(up_acc)

    def hop_mid(ch):
        for i in range(1, LINE):
            leg_line_arrival(ch, (a + i) % LINE).wait_recv()
        loop(mids, lambda i: leg_mid(ch, i).start(), 1)

    def hop_core(ch):
        loop(mids, lambda i: leg_mid_arrival(ch, (b + i) % mids).wait_recv(), 1)
        leg_core(ch).start()

    def multiply(ch):
        leg_core_arrival(ch).wait_recv()

        def block(d):
            return gathered[ch, d % CORES, (d // CORES) % mids, d // fan].astype(F32)

        stack(acc32, block, toks)
        x = acc32[...].astype(BF16)
        wg_copy(ch).wait()
        gate_acc[...] += jnp.dot(x, wg[ch], preferred_element_type=F32)
        wu_copy(ch).wait()
        up_acc[...] += jnp.dot(x, wu[ch], preferred_element_type=F32)

    def gather_step(t):
        for delay, stage in enumerate((hop_mid, hop_core, multiply)):
            pl.when((t >= delay) & (t < CHUNKS + delay))(functools.partial(stage, t - delay))

    loop(n, lambda i: share_copy(i).start(), 1)
    loop(CHUNKS + 2, gather_step)

    share_in[me] = share_out[...]
    loop(n, lambda i: share_arrival(i).wait_recv(), 1)

    stack(share_all, lambda d: share_in[d], toks)
    mine = lax.broadcasted_iota(jnp.int32, share_all.shape, 1) == me // (n // EXPERTS)
    share = jnp.sum(jnp.where(mine, share_all[...], 0.0), axis=1, keepdims=True)
    gate = gate_acc[...]
    act = (gate * jax.nn.sigmoid(gate) * up_acc[...]).astype(BF16)

    def expert_part(ch):
        wd_copy(ch).wait()
        return jnp.dot(act, wd[ch], preferred_element_type=F32) * share

    def put_out(ch, acc):
        mixed = hid[ch] + acc
        for q in range(seqs):
            out_ref[q, :, cols(ch)] = mixed[q * steps : (q + 1) * steps].astype(BF16)

    reduce_scatter(1, expert_part, put_out)

    def drain_pairs(i):
        ctx_copy(i).wait_send()
        share_copy(i).wait_send()

    loop(n, drain_pairs, 1)

    def drain_gather(ch):
        for i in range(1, LINE):
            leg_line(ch, i).wait_send()
        loop(mids, lambda i: leg_mid(ch, i).wait_send(), 1)
        leg_core(ch).wait_send()

    loop(CHUNKS, drain_gather)


def body(
    cache_kv,
    new_kv,
    queries,
    lengths,
    resid,
    value_up,
    out_proj,
    norm_gain,
    router,
    expert_ids,
    slots,
    w_gate,
    w_up,
    w_down,
):
    n = lax.axis_size("ep")
    seqs, steps, heads, kv = queries.shape
    toks = seqs * steps
    width = resid.shape[-1]
    heads_per = max(1, value_up.shape[1] // VH)
    packets = (n, toks * heads_per, LAT)
    hidden_units = w_gate.shape[1]
    mids = n // (CORES * LINE)
    part_w = width // CHUNKS
    total = n * toks
    vmem = pl.BlockSpec(memory_space=pltpu.VMEM)
    hbm = pl.BlockSpec(memory_space=pl.ANY)
    landing = [
        pltpu.VMEM((CHUNKS, mids, LINE, toks, part_w), BF16),
        pltpu.VMEM((CHUNKS, mids, LINE, toks, part_w), BF16),
        pltpu.VMEM((CHUNKS, LINE, toks, part_w), BF16),
    ]
    dma = pltpu.SemaphoreType.DMA
    mixed = pl.pallas_call(
        functools.partial(layer_kernel, n),
        out_shape=jax.ShapeDtypeStruct(resid.shape, BF16),
        in_specs=[pl.BlockSpec(memory_space=pltpu.SMEM)] + [vmem] * 5 + [hbm] * 8,
        out_specs=vmem,
        scratch_shapes=[
            pltpu.VMEM(value_up.shape, BF16),
            pltpu.VMEM((CHUNKS, out_proj.shape[0], part_w), BF16),
            pltpu.VMEM((CHUNKS, part_w, hidden_units), BF16),
            pltpu.VMEM((CHUNKS, part_w, hidden_units), BF16),
            pltpu.VMEM((CHUNKS, hidden_units, part_w), BF16),
            pltpu.VMEM((seqs, kv, cache_kv.shape[1]), BF16),
            pltpu.VMEM((seqs, 128, kv), BF16),
            pltpu.VMEM((seqs, steps * heads, kv), BF16),
            pltpu.VMEM(resid.shape, BF16),
            pltpu.VMEM((seqs, steps * heads, LAT), F32),
            pltpu.VMEM(packets, BF16),
            pltpu.VMEM(packets, BF16),
            pltpu.VMEM((n * toks * heads_per if toks * heads_per % 16 else 8, LAT), F32),
            pltpu.VMEM((total, part_w), F32),
            pltpu.VMEM((total, hidden_units), F32),
            pltpu.VMEM((total, hidden_units), F32),
            pltpu.VMEM((CHUNKS, toks, part_w), F32),
            pltpu.VMEM((CHUNKS, CORES, mids, LINE, toks, part_w), BF16),
            pltpu.VMEM((CHUNKS, mids, LINE, toks, part_w), BF16),
            pltpu.VMEM((CHUNKS, LINE, toks, part_w), BF16),
            *landing,
            *landing,
            pltpu.VMEM((CHUNKS, CORES, mids, LINE, toks, part_w), BF16),
            pltpu.VMEM((toks, 128), F32),
            pltpu.VMEM((n, toks, 128), F32),
            pltpu.VMEM((total, 128), F32),
            dma((5, CHUNKS)),
            dma((2, seqs)),
            dma((n,)),
            dma((n,)),
            dma((n,)),
            dma((n,)),
            dma((3, 2, CHUNKS)),
            dma((3, CHUNKS, mids)),
            dma((3, CHUNKS, mids)),
            dma((3, CHUNKS, LINE)),
            dma((3, CHUNKS, LINE)),
        ],
        compiler_params=pltpu.CompilerParams(
            collective_id=0, has_side_effects=True, vmem_limit_bytes=67043328
        ),
    )(
        lengths,
        new_kv,
        norm_gain.reshape(1, width),
        router.T,
        expert_ids.reshape(toks, TOP),
        slots.reshape(toks, TOP),
        cache_kv.transpose(0, 2, 1),
        queries.reshape(seqs, steps * heads, kv),
        resid,
        value_up,
        out_proj,
        w_gate,
        w_up,
        w_down,
    )
    return mixed


def solution(mesh):
    return jax.shard_map(
        body,
        mesh=mesh,
        in_specs=(
            P(("rep", "ep"), None, None),
            P(("rep", "ep"), None, None),
            P(("rep", "ep"), None, None, None),
            P(("rep", "ep")),
            P(("rep", "ep"), None, None),
            P(None, "ep"),
            P("ep", None),
            P(),
            P(),
            P(("rep", "ep"), None, None),
            P(("rep", "ep"), None, None),
            P(None, "ep"),
            P(None, "ep"),
            P("ep", None),
        ),
        out_specs=P(("rep", "ep"), None, None),
        check_vma=False,
    )
```
